32 devices in a mesh: node: 16 (over z, y, core), ell: 2 (over x).
Axes of the slice: x: 2, y: 2, z: 4, core: 2. Of those that a mesh axis runs over, the one named last changes fastest.
Arguments:
- table_zero: bfloat16 [6144, 1536], P('node', 'ell'), may hold values from -1 to 1
- table_two: bfloat16 [6144, 1536], P('node', 'ell'), may hold values from -1 to 1
- spectrum: bfloat16 [1536], P('ell'), may hold values from -0.15625 to 0.15625
- weights: float32 [6144], P('node'), may hold values from 0.02551552 to 0.25515518
Outputs:
- kernel: float32 [1536, 1536], P('node', 'ell')
The draws below stay inside these ranges and needn't reach their ends.
All inputs are finite; a program needn't handle non-finite values.
Results may differ from the reference program's by a relative error of at most 0.0029.
Values may be sent and summed in bfloat16 or wider, within the bound.
A program may use at most 128 MiB of HBM per device.

```python
import math
import jax
import jax.numpy as jnp
from jax import lax

L = 1536
NODES = 6144


def block_levels(rng, dims, split, smallest, largest):
    gain, own = 1.0, jax.random.fold_in(rng, 6)
    for dim, shards_of in split:
        heights = jnp.exp(jax.random.uniform(jax.random.fold_in(own, dim), (shards_of,), jnp.float32, smallest / len(split), largest / len(split)))
        gain = gain * jnp.repeat(heights, dims[dim] // shards_of).reshape([-1 if axis == dim else 1 for axis in range(len(dims))])
    return gain


def normal_values(stream_key, extent, deviation, most, split=(), dtype=jnp.bfloat16):
    values = deviation * jax.random.normal(stream_key, extent, jnp.float32)
    if split:
        values = values * block_levels(stream_key, extent, split, -0.22, 0.18)
    return jnp.clip(values, -most, most).astype(dtype)


def setup_inputs(seed: int = 0) -> dict:
    streams_of = jax.random.split(jax.random.key(seed), 5)
    return {
        "table_zero": jnp.clip(jax.random.uniform(streams_of[0], (NODES, L), jnp.float32, -1.0, 1.0) * block_levels(streams_of[0], (NODES, L), ((0, 16), (1, 2)), -0.4, 0.0), -1.0, 1.0).astype(jnp.bfloat16),
        "table_two": jnp.clip(jax.random.uniform(streams_of[1], (NODES, L), jnp.float32, -1.0, 1.0) * block_levels(streams_of[1], (NODES, L), ((0, 16), (1, 2)), -0.4, 0.0), -1.0, 1.0).astype(jnp.bfloat16),
        "spectrum": normal_values(streams_of[2], (L,), L ** -0.5, 0.15625, ((0, 2),)),
        "weights": jnp.clip(jnp.exp(math.log(0.25515518) - 2.30258503 * jax.random.uniform(streams_of[3], (NODES,), jnp.float32) ** block_levels(streams_of[3], (NODES,), ((0, 16),), -0.2, 0.2)), 0.02551552, 0.25515518),
    }


def reference(table_zero, table_two, spectrum, weights):
    xi = jnp.dot(table_zero, spectrum, preferred_element_type=jnp.float32)
    weighted = ((weights * xi)[:, None] * table_zero.astype(jnp.float32)).astype(jnp.bfloat16)
    return lax.dot_general(weighted, table_two, (((0,), (0,)), ((), ())), preferred_element_type=jnp.float32)
```

```python
import functools

import jax
import jax.numpy as jnp
from jax import lax
from jax.experimental import pallas as pl
from jax.experimental.pallas import tpu as pltpu
from jax.sharding import PartitionSpec as P

MESH = pl.DeviceIdType.MESH
F32, BF16 = jnp.float32, jnp.bfloat16
SPLIT = 2


def kernel(nodes, ells, rows, tz, t2, spec, wts, out, gath, xsnd, xrcv, part, cbuf,
           ysnd, yrcv, zsnd, zrcv, g_s, g_r, x_s, x_r, c_s, c_r, y_s, y_r, z_s, z_r):
    depth, half = tz.shape
    zs_all, wide = nodes // 4, 4 * rows
    per = half // wide
    cols = t2.shape[1] // SPLIT
    n, e = lax.axis_index("node"), lax.axis_index("ell")
    c, y, z = lax.rem(n, 2), lax.rem(n // 2, 2), n // 4

    def at(zz, yy, cc):
        return (zz * 4 + yy * 2 + cc, e)

    def peer(d):
        return lax.rem(e + d, ells)

    def order(i, src):
        return jnp.where(src < ells // 2, i, per - 1 - i)

    barrier = pltpu.get_barrier_semaphore()
    greet = [(n, peer(d)) for d in range(1, ells)]
    greet += [at(z, y, 1 - c), at(z, 1 - y, c)]
    greet += [at(lax.rem(z + d, zs_all), y, c) for d in range(1, zs_all)]
    for device in greet:
        pl.semaphore_signal(barrier, inc=1, device_id=device, device_id_type=MESH)

    xsnd[...] = lax.dot_general(
        jnp.broadcast_to(spec[...], (16, half)), tz[...], (((1,), (1,)), ((), ())),
        preferred_element_type=F32)[:8]
    pl.semaphore_wait(barrier, len(greet))

    def remote(src, dst, s_sem, r_sem, device):
        return pltpu.make_async_remote_copy(
            src_ref=src, dst_ref=dst, send_sem=s_sem, recv_sem=r_sem,
            device_id=device, device_id_type=MESH)

    xi_copies, g_copies = [], {}
    for d in range(1, ells):
        xi_copies.append(remote(xsnd, xrcv.at[d - 1], x_s.at[d - 1], x_r.at[d - 1], (n, peer(d))))
        xi_copies[-1].start()
    for i in range(per):
        for d in range(1, ells):
            start = pl.multiple_of(order(i, e) * wide, 128)
            g_copies[d, i] = remote(
                tz.at[:, pl.ds(start, wide)], gath.at[d - 1, i],
                g_s.at[d - 1, i], g_r.at[d - 1, i], (n, peer(d)))
            g_copies[d, i].start()

    xi = xsnd[...]
    for d in range(1, ells):
        xi_copies[d - 1].wait_recv()
        xi = xi + xrcv[d - 1]
    scale = jnp.transpose(xi * wts[...])[:, 0:1]

    c_copies, y_copies, goal = {}, {}, {}

    def multiply(j):
        d, i = j // per, j % per
        src = lax.rem(e + ells - d, ells)
        goal[j] = src * per + order(i, src)
        if d == 0:
            raw = tz[:, pl.ds(pl.multiple_of(order(i, e) * wide, 128), wide)]
        else:
            g_copies[d, i].wait_recv()
            raw = gath[d - 1, i]
        weighted = (scale * raw.astype(F32)).astype(BF16)
        for s in range(SPLIT):
            prod = lax.dot_general(
                weighted, t2[:, s * cols:(s + 1) * cols], (((0,), (0,)), ((), ())),
                preferred_element_type=F32)
            for cc in range(2):
                for yy in range(2):
                    k = (2 * yy + cc) * rows
                    part[j, s, cc, yy] = prod[k:k + rows]
            c_copies[j, s] = remote(
                part.at[j, s, 1 - c], cbuf.at[j, s], c_s.at[j, s], c_r.at[j, s],
                at(z, y, 1 - c))
            c_copies[j, s].start()

    def over_y(j):
        for s in range(SPLIT):
            c_copies[j, s].wait_recv()
            ysnd[j, s] = (part[j, s, c, 1 - y] + cbuf[j, s, 1 - y]).astype(BF16)
            y_copies[j, s] = remote(
                ysnd.at[j, s], yrcv.at[j, s], y_s.at[j, s], y_r.at[j, s], at(z, 1 - y, c))
            y_copies[j, s].start()

    def z_copy(j, s):
        return remote(zsnd.at[j, s], zrcv.at[z, s], z_s.at[j, s], z_r.at[z, s], at(goal[j], y, c))

    def over_z(j):
        for s in range(SPLIT):
            y_copies[j, s].wait_recv()
            total = part[j, s, c, y] + cbuf[j, s, y] + yrcv[j, s].astype(F32)

            @pl.when(goal[j] == z)
            def _():
                out[:, s * cols:(s + 1) * cols] = total

            @pl.when(goal[j] != z)
            def _():
                zsnd[j, s] = total.astype(BF16)
                z_copy(j, s).start()

    for j in range(per):
        multiply(j)
    for j in range(per):
        over_y(j)
    pending = list(range(per))
    for j in range(per, zs_all):
        multiply(j)
        over_y(j)
        for k in pending:
            over_z(k)
        pending = [j]
    for k in pending:
        over_z(k)

    for s in range(SPLIT):
        for k in range(zs_all):
            @pl.when(k != z)
            def _():
                remote(zsnd.at[0, s], zrcv.at[k, s], z_s.at[0, s], z_r.at[k, s], at(k, y, c)).wait_recv()
                out[:, s * cols:(s + 1) * cols] += zrcv[k, s].astype(F32)

    for copy in xi_copies + list(g_copies.values()) + list(c_copies.values()) + list(y_copies.values()):
        copy.wait_send()
    for j in range(zs_all):
        for s in range(SPLIT):
            @pl.when(goal[j] != z)
            def _():
                z_copy(j, s).wait_send()


def per_device(nodes, ells, table_zero, table_two, spectrum, weights):
    depth, half = table_zero.shape
    rows = half * ells // nodes
    width = table_two.shape[1]
    zs_all, per, cols = nodes // 4, half // (4 * rows), width // SPLIT
    peers = max(ells - 1, 1)
    dma = pltpu.SemaphoreType.DMA
    vmem = pl.BlockSpec(memory_space=pltpu.VMEM)
    return pl.pallas_call(
        functools.partial(kernel, nodes, ells, rows),
        out_shape=jax.ShapeDtypeStruct((rows, width), F32),
        in_specs=[vmem] * 4,
        out_specs=vmem,
        scratch_shapes=[
            pltpu.VMEM((peers, per, depth, 4 * rows), BF16),
            pltpu.VMEM((8, depth), F32),
            pltpu.VMEM((peers, 8, depth), F32),
            pltpu.VMEM((zs_all, SPLIT, 2, 2, rows, cols), F32),
            pltpu.VMEM((zs_all, SPLIT, 2, rows, cols), F32),
            pltpu.VMEM((zs_all, SPLIT, rows, cols), BF16),
            pltpu.VMEM((zs_all, SPLIT, rows, cols), BF16),
            pltpu.VMEM((zs_all, SPLIT, rows, cols), BF16),
            pltpu.VMEM((zs_all, SPLIT, rows, cols), BF16),
            dma((peers, per)), dma((peers, per)),
            dma((peers,)), dma((peers,)),
            dma((zs_all, SPLIT)), dma((zs_all, SPLIT)),
            dma((zs_all, SPLIT)), dma((zs_all, SPLIT)),
            dma((zs_all, SPLIT)), dma((zs_all, SPLIT)),
        ],
        compiler_params=pltpu.CompilerParams(
            collective_id=0, has_side_effects=True, vmem_limit_bytes=60 * 1024 * 1024),
    )(table_zero, table_two, spectrum.reshape(1, half), weights.reshape(1, depth))


def solution(mesh):
    placed = (P("node", "ell"), P("node", "ell"), P("ell"), P("node"))
    return jax.shard_map(
        functools.partial(per_device, mesh.shape["node"], mesh.shape["ell"]),
        mesh=mesh, in_specs=placed, out_specs=P("node", "ell"), check_vma=False)
```

```python
import functools

import jax
import jax.numpy as jnp
from jax import lax
from jax.experimental import pallas as pl
from jax.experimental.pallas import tpu as pltpu
from jax.sharding import PartitionSpec as P

MESH = pl.DeviceIdType.MESH
F32, BF16 = jnp.float32, jnp.bfloat16
PARTS = 3


def kernel(nodes, ells, rows, tz_hbm, t2_hbm, spec, wts, out, tz, t2, own, gath, xsnd, xrcv,
           part, cbuf, ysnd, yrcv, zsnd, zrcv, in_s, g_s, g_r, x_s, x_r, c_s, c_r,
           y_s, y_r, z_s, z_r):
    depth, half = tz.shape
    zs_all, wide, sub = nodes // 4, 4 * rows, rows // PARTS
    slabs = half // wide
    per = slabs * PARTS
    n, e = lax.axis_index("node"), lax.axis_index("ell")
    c, y, z = lax.rem(n, 2), lax.rem(n // 2, 2), n // 4

    def at(zz, yy, cc):
        return (zz * 4 + yy * 2 + cc, e)

    def peer(d):
        return lax.rem(e + d, ells)

    def order(q, src):
        return jnp.where(src < ells // 2, q, slabs - 1 - q)

    loads = [pltpu.make_async_copy(tz_hbm, tz, in_s.at[0]),
             pltpu.make_async_copy(t2_hbm, t2, in_s.at[1])]
    for load in loads:
        load.start()
    barrier = pltpu.get_barrier_semaphore()
    greet = [(n, peer(d)) for d in range(1, ells)]
    greet += [at(z, y, 1 - c), at(z, 1 - y, c)]
    greet += [at(lax.rem(z + d, zs_all), y, c) for d in range(1, zs_all)]
    for device in greet:
        pl.semaphore_signal(barrier, inc=1, device_id=device, device_id_type=MESH)

    def remote(src, dst, s_sem, r_sem, device):
        return pltpu.make_async_remote_copy(
            src_ref=src, dst_ref=dst, send_sem=s_sem, recv_sem=r_sem,
            device_id=device, device_id_type=MESH)

    loads[0].wait()
    xsnd[...] = lax.dot_general(
        jnp.broadcast_to(spec[...].reshape(1, half), (16, half)), tz[...],
        (((1,), (1,)), ((), ())), preferred_element_type=F32)[:8]

    xi_copies, g_copies = [], {}
    for q in range(slabs):
        start = pl.multiple_of(order(q, e) * wide, 128)
        turned = jnp.transpose(tz[:, pl.ds(start, wide)])
        for t in range(PARTS):
            for k in range(4):
                low = k * rows + t * sub
                own[q * PARTS + t, k * sub:(k + 1) * sub] = turned[low:low + sub]
        if q == 0:
            pl.semaphore_wait(barrier, len(greet))
            for d in range(1, ells):
                xi_copies.append(remote(
                    xsnd, xrcv.at[d - 1], x_s.at[d - 1], x_r.at[d - 1], (n, peer(d))))
                xi_copies[-1].start()
        for i in range(q * PARTS, (q + 1) * PARTS):
            for d in range(1, ells):
                g_copies[d, i] = remote(
                    own.at[i], gath.at[d - 1, i], g_s.at[d - 1, i], g_r.at[d - 1, i],
                    (n, peer(d)))
                g_copies[d, i].start()

    xi = xsnd[...]
    for d in range(1, ells):
        xi_copies[d - 1].wait_recv()
        xi = xi + xrcv[d - 1]
    scale = xi[0:1] * wts[...].reshape(1, depth)
    loads[1].wait()

    c_copies, y_copies, goal = {}, {}, {}

    def multiply(j):
        d, i = j // per, j % per
        src = lax.rem(e + ells - d, ells)
        goal[j] = src * slabs + order(i // PARTS, src)
        if d == 0:
            raw = own[i]
        else:
            g_copies[d, i].wait_recv()
            raw = gath[d - 1, i]
        weighted = (scale * raw.astype(F32)).astype(BF16)
        prod = jnp.dot(weighted, t2[...], preferred_element_type=F32)
        for cc in range(2):
            for yy in range(2):
                k = (2 * yy + cc) * sub
                part[j, cc, yy] = prod[k:k + sub]
        c_copies[j] = remote(
            part.at[j, 1 - c], cbuf.at[j], c_s.at[j], c_r.at[j], at(z, y, 1 - c))
        c_copies[j].start()

    def over_y(j):
        c_copies[j].wait_recv()
        ysnd[j] = (part[j, c, 1 - y] + cbuf[j, 1 - y]).astype(BF16)
        y_copies[j] = remote(ysnd.at[j], yrcv.at[j], y_s.at[j], y_r.at[j], at(z, 1 - y, c))
        y_copies[j].start()

    def z_copy(j):
        t = j % PARTS
        return remote(zsnd.at[j], zrcv.at[z, t], z_s.at[j], z_r.at[z, t], at(goal[j], y, c))

    def over_z(j):
        t = j % PARTS
        y_copies[j].wait_recv()
        total = part[j, c, y] + cbuf[j, y] + yrcv[j].astype(F32)

        @pl.when(goal[j] == z)
        def _():
            out[t * sub:(t + 1) * sub] = total

        @pl.when(goal[j] != z)
        def _():
            zsnd[j] = total.astype(BF16)
            z_copy(j).start()

    count = zs_all * PARTS
    for j in range(per):
        multiply(j)
        if j:
            over_y(j - 1)
    over_y(per - 1)
    pending = list(range(per))
    for j in range(per, count):
        multiply(j)
        over_y(j)
        for _ in range(min(2, len(pending))):
            over_z(pending.pop(0))
        pending.append(j)
    for j in pending:
        over_z(j)

    for t in range(PARTS):
        for k in range(zs_all):
            @pl.when(k != z)
            def _():
                remote(zsnd.at[t], zrcv.at[k, t], z_s.at[t], z_r.at[k, t], at(k, y, c)).wait_recv()
                out[t * sub:(t + 1) * sub] += zrcv[k, t].astype(F32)

    for copy in xi_copies + list(g_copies.values()) + list(c_copies.values()) + list(y_copies.values()):
        copy.wait_send()
    for j in range(count):
        @pl.when(goal[j] != z)
        def _():
            z_copy(j).wait_send()


def per_device(nodes, ells, table_zero, table_two, spectrum, weights):
    depth, half = table_zero.shape
    rows = half * ells // nodes
    width = table_two.shape[1]
    slabs, sub, peers = half // (4 * rows), rows // PARTS, max(ells - 1, 1)
    per, count = slabs * PARTS, nodes // 4 * PARTS
    dma = pltpu.SemaphoreType.DMA
    vmem = pl.BlockSpec(memory_space=pltpu.VMEM)
    anywhere = pl.BlockSpec(memory_space=pl.ANY)
    return pl.pallas_call(
        functools.partial(kernel, nodes, ells, rows),
        out_shape=jax.ShapeDtypeStruct((rows, width), F32),
        in_specs=[anywhere, anywhere, vmem, vmem],
        out_specs=vmem,
        scratch_shapes=[
            pltpu.VMEM((depth, half), BF16),
            pltpu.VMEM((depth, width), BF16),
            pltpu.VMEM((per, 4 * sub, depth), BF16),
            pltpu.VMEM((peers, per, 4 * sub, depth), BF16),
            pltpu.VMEM((8, depth), F32),
            pltpu.VMEM((peers, 8, depth), F32),
            pltpu.VMEM((count, 2, 2, sub, width), F32),
            pltpu.VMEM((count, 2, sub, width), F32),
            pltpu.VMEM((count, sub, width), BF16),
            pltpu.VMEM((count, sub, width), BF16),
            pltpu.VMEM((count, sub, width), BF16),
            pltpu.VMEM((nodes // 4, PARTS, sub, width), BF16),
            dma((2,)),
            dma((peers, per)), dma((peers, per)),
            dma((peers,)), dma((peers,)),
            dma((count,)), dma((count,)),
            dma((count,)), dma((count,)),
            dma((count,)), dma((nodes // 4, PARTS)),
        ],
        compiler_params=pltpu.CompilerParams(
            collective_id=0, has_side_effects=True, vmem_limit_bytes=60 * 1024 * 1024),
    )(table_zero, table_two, spectrum, weights)


def solution(mesh):
    placed = (P("node", "ell"), P("node", "ell"), P("ell"), P("node"))
    return jax.shard_map(
        functools.partial(per_device, mesh.shape["node"], mesh.shape["ell"]),
        mesh=mesh, in_specs=placed, out_specs=P("node", "ell"), check_vma=False)
```

```python
import functools

import jax
import jax.numpy as jnp
from jax import lax
from jax.experimental import pallas as pl
from jax.experimental.pallas import tpu as pltpu
from jax.sharding import PartitionSpec as P

MESH = pl.DeviceIdType.MESH
F32, BF16 = jnp.float32, jnp.bfloat16
PARTS = 3


def kernel(nodes, ells, rows, tz_hbm, t2_hbm, spec, wts, out, tz, t2, own, gath, xsnd, xrcv,
           part, cbuf, ysnd, yrcv, zsnd, zrcv, in_s, g_s, g_r, x_s, x_r, c_s, c_r,
           y_s, y_r, z_s, z_r):
    depth, half = tz.shape
    zs_all, wide, sub = nodes // 4, 4 * rows, rows // PARTS
    slabs = half // wide
    per = slabs * PARTS
    n, e = lax.axis_index("node"), lax.axis_index("ell")
    c, y, z = lax.rem(n, 2), lax.rem(n // 2, 2), n // 4

    def at(zz, yy, cc):
        return (zz * 4 + yy * 2 + cc, e)

    def peer(d):
        return lax.rem(e + d, ells)

    def order(q, src):
        return jnp.where(src < ells // 2, q, slabs - 1 - q)

    loads = [pltpu.make_async_copy(tz_hbm, tz, in_s.at[0]),
             pltpu.make_async_copy(t2_hbm, t2, in_s.at[1])]
    for load in loads:
        load.start()
    barrier = pltpu.get_barrier_semaphore()
    greet = [(n, peer(d)) for d in range(1, ells)]
    greet += [at(z, y, 1 - c), at(z, 1 - y, c)]
    greet += [at(lax.rem(z + d, zs_all), y, c) for d in range(1, zs_all)]
    for device in greet:
        pl.semaphore_signal(barrier, inc=1, device_id=device, device_id_type=MESH)

    def remote(src, dst, s_sem, r_sem, device):
        return pltpu.make_async_remote_copy(
            src_ref=src, dst_ref=dst, send_sem=s_sem, recv_sem=r_sem,
            device_id=device, device_id_type=MESH)

    loads[0].wait()
    xsnd[...] = lax.dot_general(
        jnp.broadcast_to(spec[...].reshape(1, half), (16, half)), tz[...],
        (((1,), (1,)), ((), ())), preferred_element_type=F32)[:8]

    xi_copies, g_copies = [], {}
    for q in range(slabs):
        start = pl.multiple_of(order(q, e) * wide, 128)
        turned = jnp.transpose(tz[:, pl.ds(start, wide)])
        for t in range(PARTS):
            for k in range(4):
                low = k * rows + t * sub
                own[q * PARTS + t, k * sub:(k + 1) * sub] = turned[low:low + sub]
        if q == 0:
            pl.semaphore_wait(barrier, len(greet))
            for d in range(1, ells):
                xi_copies.append(remote(
                    xsnd, xrcv.at[d - 1], x_s.at[d - 1], x_r.at[d - 1], (n, peer(d))))
                xi_copies[-1].start()
        for i in range(q * PARTS, (q + 1) * PARTS):
            for d in range(1, ells):
                g_copies[d, i] = remote(
                    own.at[i], gath.at[d - 1, i], g_s.at[d - 1, i], g_r.at[d - 1, i],
                    (n, peer(d)))
                g_copies[d, i].start()

    xi = xsnd[...]
    for d in range(1, ells):
        xi_copies[d - 1].wait_recv()
        xi = xi + xrcv[d - 1]
    scale = xi[0:1] * wts[...].reshape(1, depth)
    loads[1].wait()

    c_copies, y_copies, goal = {}, {}, {}

    def multiply(j):
        d, i = j // per, j % per
        src = lax.rem(e + ells - d, ells)
        goal[j] = src * slabs + order(i // PARTS, src)
        if d == 0:
            raw = own[i]
        else:
            g_copies[d, i].wait_recv()
            raw = gath[d - 1, i]
        weighted = (scale * raw.astype(F32)).astype(BF16)
        prod = jnp.dot(weighted, t2[...], preferred_element_type=F32)
        for cc in range(2):
            for yy in range(2):
                k = (2 * yy + cc) * sub
                part[j, cc, yy] = prod[k:k + sub]
        c_copies[j] = remote(
            part.at[j, 1 - c], cbuf.at[j], c_s.at[j], c_r.at[j], at(z, y, 1 - c))
        c_copies[j].start()

    def over_y(j):
        c_copies[j].wait_recv()
        ysnd[j] = (part[j, c, 1 - y] + cbuf[j, 1 - y]).astype(BF16)
        y_copies[j] = remote(ysnd.at[j], yrcv.at[j], y_s.at[j], y_r.at[j], at(z, 1 - y, c))
        y_copies[j].start()

    def z_copy(j):
        t = j % PARTS
        return remote(zsnd.at[j], zrcv.at[z, t], z_s.at[j], z_r.at[z, t], at(goal[j], y, c))

    def over_z(j):
        t = j % PARTS
        y_copies[j].wait_recv()
        total = part[j, c, y] + cbuf[j, y] + yrcv[j].astype(F32)

        @pl.when(goal[j] == z)
        def _():
            out[t * sub:(t + 1) * sub] = total

        @pl.when(goal[j] != z)
        def _():
            zsnd[j] = total.astype(BF16)
            z_copy(j).start()

    count = zs_all * PARTS
    for j in range(per):
        multiply(j)
    sent, mine = [], list(range(per))

    def next_y(j):
        over_y(j)
        sent.append(j)

    for _ in range(min(2, per)):
        next_y(mine.pop(0))
    for j in range(per, count):
        multiply(j)
        if j > per + 1 and len(sent) > 1:
            over_z(sent.pop(0))
        next_y(j)
        if mine:
            next_y(mine.pop(0))
        if j > per and len(sent) > 1:
            over_z(sent.pop(0))
    for j in mine:
        next_y(j)
    for j in sent:
        over_z(j)

    for t in range(PARTS):
        for k in range(zs_all):
            @pl.when(k != z)
            def _():
                remote(zsnd.at[t], zrcv.at[k, t], z_s.at[t], z_r.at[k, t], at(k, y, c)).wait_recv()
                out[t * sub:(t + 1) * sub] += zrcv[k, t].astype(F32)

    for copy in xi_copies + list(g_copies.values()) + list(c_copies.values()) + list(y_copies.values()):
        copy.wait_send()
    for j in range(count):
        @pl.when(goal[j] != z)
        def _():
            z_copy(j).wait_send()


def per_device(nodes, ells, table_zero, table_two, spectrum, weights):
    depth, half = table_zero.shape
    rows = half * ells // nodes
    width = table_two.shape[1]
    slabs, sub, peers = half // (4 * rows), rows // PARTS, max(ells - 1, 1)
    per, count = slabs * PARTS, nodes // 4 * PARTS
    dma = pltpu.SemaphoreType.DMA
    vmem = pl.BlockSpec(memory_space=pltpu.VMEM)
    anywhere = pl.BlockSpec(memory_space=pl.ANY)
    return pl.pallas_call(
        functools.partial(kernel, nodes, ells, rows),
        out_shape=pltpu.VMEM((rows, width), F32),
        in_specs=[anywhere, anywhere, vmem, vmem],
        out_specs=vmem,
        scratch_shapes=[
            pltpu.VMEM((depth, half), BF16),
            pltpu.VMEM((depth, width), BF16),
            pltpu.VMEM((per, 4 * sub, depth), BF16),
            pltpu.VMEM((peers, per, 4 * sub, depth), BF16),
            pltpu.VMEM((8, depth), F32),
            pltpu.VMEM((peers, 8, depth), F32),
            pltpu.VMEM((count, 2, 2, sub, width), F32),
            pltpu.VMEM((count, 2, sub, width), F32),
            pltpu.VMEM((count, sub, width), BF16),
            pltpu.VMEM((count, sub, width), BF16),
            pltpu.VMEM((count, sub, width), BF16),
            pltpu.VMEM((nodes // 4, PARTS, sub, width), BF16),
            dma((2,)),
            dma((peers, per)), dma((peers, per)),
            dma((peers,)), dma((peers,)),
            dma((count,)), dma((count,)),
            dma((count,)), dma((count,)),
            dma((count,)), dma((nodes // 4, PARTS)),
        ],
        compiler_params=pltpu.CompilerParams(
            collective_id=0, has_side_effects=True, vmem_limit_bytes=60 * 1024 * 1024),
    )(table_zero, table_two, spectrum, weights)


def solution(mesh):
    placed = (P("node", "ell"), P("node", "ell"), P("ell"), P("node"))
    return jax.shard_map(
        functools.partial(per_device, mesh.shape["node"], mesh.shape["ell"]),
        mesh=mesh, in_specs=placed, out_specs=P("node", "ell"), check_vma=False)
```

```python
import functools

import jax
import jax.numpy as jnp
from jax import lax
from jax.experimental import pallas as pl
from jax.experimental.pallas import tpu as pltpu
from jax.sharding import PartitionSpec as P

MESH = pl.DeviceIdType.MESH
F32, BF16 = jnp.float32, jnp.bfloat16
PARTS = 3


def kernel(nodes, ells, rows, tz_hbm, t2_hbm, spec, wts, out, tz, t2, own, gath, xsnd, xrcv,
           part, cbuf, ysnd, yrcv, zsnd, zrcv, in_s, g_s, g_r, x_s, x_r, c_s, c_r,
           y_s, y_r, z_s, z_r):
    depth, half = tz.shape
    zs_all, wide, sub = nodes // 4, 4 * rows, rows // PARTS
    slabs = half // wide
    per = slabs * PARTS
    n, e = lax.axis_index("node"), lax.axis_index("ell")
    c, y, z = lax.rem(n, 2), lax.rem(n // 2, 2), n // 4

    def at(zz, yy, cc):
        return (zz * 4 + yy * 2 + cc, e)

    def peer(d):
        return lax.rem(e + d, ells)

    def order(q, src):
        return jnp.where(src < ells // 2, q, slabs - 1 - q)

    loads = [pltpu.make_async_copy(tz_hbm, tz, in_s.at[0]),
             pltpu.make_async_copy(t2_hbm, t2, in_s.at[1])]
    for load in loads:
        load.start()
    barrier = pltpu.get_barrier_semaphore()
    greet = [(n, peer(d)) for d in range(1, ells)]
    greet += [at(z, y, 1 - c), at(z, 1 - y, c)]
    greet += [at(lax.rem(z + d, zs_all), y, c) for d in range(1, zs_all)]
    for device in greet:
        pl.semaphore_signal(barrier, inc=1, device_id=device, device_id_type=MESH)

    def remote(src, dst, s_sem, r_sem, device):
        return pltpu.make_async_remote_copy(
            src_ref=src, dst_ref=dst, send_sem=s_sem, recv_sem=r_sem,
            device_id=device, device_id_type=MESH)

    loads[0].wait()
    xsnd[...] = lax.dot_general(
        jnp.broadcast_to(spec[...].reshape(1, half), (16, half)), tz[...],
        (((1,), (1,)), ((), ())), preferred_element_type=F32)[:1]

    xi_copies, g_copies = [], {}
    for q in range(slabs):
        start = pl.multiple_of(order(q, e) * wide, 128)
        turned = jnp.transpose(tz[:, pl.ds(start, wide)])
        for t in range(PARTS):
            for k in range(4):
                low = k * rows + t * sub
                own[q * PARTS + t, k * sub:(k + 1) * sub] = turned[low:low + sub]
        if q == 0:
            pl.semaphore_wait(barrier, len(greet))
            for d in range(1, ells):
                xi_copies.append(remote(
                    xsnd, xrcv.at[d - 1], x_s.at[d - 1], x_r.at[d - 1], (n, peer(d))))
                xi_copies[-1].start()
        for i in range(q * PARTS, (q + 1) * PARTS):
            for d in range(1, ells):
                g_copies[d, i] = remote(
                    own.at[i], gath.at[d - 1, i], g_s.at[d - 1, i], g_r.at[d - 1, i],
                    (n, peer(d)))
                g_copies[d, i].start()

    xi = xsnd[...]
    for d in range(1, ells):
        xi_copies[d - 1].wait_recv()
        xi = xi + xrcv[d - 1]
    scale = xi[0:1] * wts[...].reshape(1, depth)
    loads[1].wait()

    c_copies, y_copies, goal = {}, {}, {}

    def multiply(j):
        d, i = j // per, j % per
        src = lax.rem(e + ells - d, ells)
        goal[j] = src * slabs + order(i // PARTS, src)
        if d == 0:
            raw = own[i]
        else:
            g_copies[d, i].wait_recv()
            raw = gath[d - 1, i]
        weighted = (scale * raw.astype(F32)).astype(BF16)
        prod = jnp.dot(weighted, t2[...], preferred_element_type=F32)
        for cc in range(2):
            for yy in range(2):
                k = (2 * yy + cc) * sub
                part[j, cc, yy] = prod[k:k + sub]
        c_copies[j] = remote(
            part.at[j, 1 - c], cbuf.at[j], c_s.at[j], c_r.at[j], at(z, y, 1 - c))
        c_copies[j].start()

    def over_y(j):
        c_copies[j].wait_recv()
        ysnd[j] = (part[j, c, 1 - y] + cbuf[j, 1 - y]).astype(BF16)
        y_copies[j] = remote(ysnd.at[j], yrcv.at[j], y_s.at[j], y_r.at[j], at(z, 1 - y, c))
        y_copies[j].start()

    def z_copy(j):
        t = j % PARTS
        return remote(zsnd.at[j], zrcv.at[z, t], z_s.at[j], z_r.at[z, t], at(goal[j], y, c))

    def over_z(j):
        t = j % PARTS
        y_copies[j].wait_recv()
        total = part[j, c, y] + cbuf[j, y] + yrcv[j].astype(F32)

        @pl.when(goal[j] == z)
        def _():
            out[t * sub:(t + 1) * sub] = total

        @pl.when(goal[j] != z)
        def _():
            zsnd[j] = total.astype(BF16)
            z_copy(j).start()

    count = zs_all * PARTS
    for j in range(per):
        multiply(j)
    sent, mine = [], list(range(per))

    def next_y(j):
        over_y(j)
        sent.append(j)

    for _ in range(min(1, per)):
        next_y(mine.pop(0))
    for j in range(per, count):
        multiply(j)
        if j > per + 1 and len(sent) > 1:
            over_z(sent.pop(0))
        next_y(j)
        if mine:
            next_y(mine.pop(0))
        if j > per and len(sent) > 1:
            over_z(sent.pop(0))
    for j in mine:
        next_y(j)
    for j in sent:
        over_z(j)

    for t in range(PARTS):
        for k in range(zs_all):
            @pl.when(k != z)
            def _():
                remote(zsnd.at[t], zrcv.at[k, t], z_s.at[t], z_r.at[k, t], at(k, y, c)).wait_recv()
                out[t * sub:(t + 1) * sub] += zrcv[k, t].astype(F32)

    for copy in xi_copies + list(g_copies.values()) + list(c_copies.values()) + list(y_copies.values()):
        copy.wait_send()
    for j in range(count):
        @pl.when(goal[j] != z)
        def _():
            z_copy(j).wait_send()


def per_device(nodes, ells, table_zero, table_two, spectrum, weights):
    depth, half = table_zero.shape
    rows = half * ells // nodes
    width = table_two.shape[1]
    slabs, sub, peers = half // (4 * rows), rows // PARTS, max(ells - 1, 1)
    per, count = slabs * PARTS, nodes // 4 * PARTS
    dma = pltpu.SemaphoreType.DMA
    vmem = pl.BlockSpec(memory_space=pltpu.VMEM)
    anywhere = pl.BlockSpec(memory_space=pl.ANY)
    return pl.pallas_call(
        functools.partial(kernel, nodes, ells, rows),
        out_shape=pltpu.VMEM((rows, width), F32),
        in_specs=[anywhere, anywhere, vmem, vmem],
        out_specs=vmem,
        scratch_shapes=[
            pltpu.VMEM((depth, half), BF16),
            pltpu.VMEM((depth, width), BF16),
            pltpu.VMEM((per, 4 * sub, depth), BF16),
            pltpu.VMEM((peers, per, 4 * sub, depth), BF16),
            pltpu.VMEM((1, depth), F32),
            pltpu.VMEM((peers, 1, depth), F32),
            pltpu.VMEM((count, 2, 2, sub, width), F32),
            pltpu.VMEM((count, 2, sub, width), F32),
            pltpu.VMEM((count, sub, width), BF16),
            pltpu.VMEM((count, sub, width), BF16),
            pltpu.VMEM((count, sub, width), BF16),
            pltpu.VMEM((nodes // 4, PARTS, sub, width), BF16),
            dma((2,)),
            dma((peers, per)), dma((peers, per)),
            dma((peers,)), dma((peers,)),
            dma((count,)), dma((count,)),
            dma((count,)), dma((count,)),
            dma((count,)), dma((nodes // 4, PARTS)),
        ],
        compiler_params=pltpu.CompilerParams(
            collective_id=0, has_side_effects=True, vmem_limit_bytes=60 * 1024 * 1024),
    )(table_zero, table_two, spectrum, weights)


def solution(mesh):
    placed = (P("node", "ell"), P("node", "ell"), P("ell"), P("node"))
    return jax.shard_map(
        functools.partial(per_device, mesh.shape["node"], mesh.shape["ell"]),
        mesh=mesh, in_specs=placed, out_specs=P("node", "ell"), check_vma=False)
```
